32 devices in a mesh: gx: 4 (over y, x), gy: 2 (over core), gz: 4 (over z).
Axes of the slice: x: 2, y: 2, z: 4, core: 2. Of those that a mesh axis runs over, the one named last changes fastest.
Arguments:
- params: float32 [12, 7168, 1536], P('gx', 'gy', 'gz'), may hold values from -100 to 100
- grads: bfloat16 [12, 7168, 1536], P('gx', 'gy', 'gz'), may hold values from -300 to 300
- row_state: float32 [12, 7168], P('gx', 'gy'), may hold values from 0.01 to 1
- col_state: float32 [12, 1536], P('gx', 'gz'), may hold values from 0.01 to 1
Outputs:
- new_params: float32 [12, 7168, 1536], P('gx', 'gy', 'gz')
- row_new: float32 [12, 7168], P('gx', 'gy')
- col_new: float32 [12, 1536], P('gx', 'gz')
- applied_step: float32 [12, 7168, 1536], P('gx', 'gy', 'gz')
- compute_copy: bfloat16 [12, 7168, 1536], P('gx', 'gy')
The draws below stay inside these ranges and needn't reach their ends.
All inputs are finite; a program needn't handle non-finite values.
Results may differ from the reference program's by a relative error of at most 0.0004.
Values may be sent and summed in bfloat16 or wider, within the bound.
A program may use at most 192 MiB of HBM per device.

```python
import math
import jax
import jax.numpy as jnp
from jax import lax

D = 7168
QR = 1536
LAY = 12


def draw_params(key, part):
    subkeys = jax.random.split(jax.random.fold_in(key, 17), 3)
    normal_part = jnp.clip(jax.random.normal(subkeys[0], (LAY, D, QR), jnp.float32), -6.0, 6.0)
    row_rise = jnp.arange(D, dtype=jnp.float32) / D
    col_rise = jnp.arange(QR, dtype=jnp.float32) / QR
    row_scale = 10.0 ** (0.5 * row_rise + 0.4 * jax.random.uniform(subkeys[1], (D,), jnp.float32) - 0.45)
    col_scale = 10.0 ** (0.5 * col_rise + 0.4 * jax.random.uniform(subkeys[2], (QR,), jnp.float32) - 0.45)
    weights = normal_part * row_scale[None, :, None] * col_scale[None, None, :]
    return weights.astype(jnp.float32)


def draw_grads(key, part):
    subkeys = jax.random.split(key, 3)
    normal_part = jnp.clip(jax.random.normal(subkeys[0], (LAY, D, QR), jnp.float32), -6.0, 6.0)
    row_rise = jnp.arange(D, dtype=jnp.float32) / D
    col_rise = jnp.arange(QR, dtype=jnp.float32) / QR
    layer_rise = jnp.arange(LAY, dtype=jnp.float32) / LAY
    row_scale = 10.0 ** (0.5 * row_rise + 0.5 * jax.random.uniform(subkeys[1], (D,), jnp.float32) - 0.5)
    col_scale = 10.0 ** (0.5 * col_rise + 0.5 * jax.random.uniform(subkeys[2], (QR,), jnp.float32) - 0.5)
    layer_scale = 10.0 ** (0.25 * layer_rise)
    gradient = normal_part * row_scale[None, :, None] * col_scale[None, None, :] * layer_scale[:, None, None]
    return gradient.astype(jnp.bfloat16)


def steps_of(own_key, dims, shards, least, top_value):
    def one(dim, shards_of):
        draws = jax.random.uniform(jax.random.fold_in(jax.random.fold_in(own_key, 6), dim), (shards_of,), jnp.float32, least / len(shards), top_value / len(shards))
        return jnp.repeat(jnp.exp(draws), dims[dim] // shards_of).reshape((-1,) + (1,) * (len(dims) - dim - 1))

    level = one(*shards[0])
    for cut in shards[1:]:
        level = level * one(*cut)
    return level


def setup_inputs(seed: int = 0) -> dict:
    streams_of = jax.random.split(jax.random.key(seed), 5)
    return {
        "params": draw_params(jax.random.fold_in(streams_of[4], 71), 0),
        "grads": draw_grads(jax.random.fold_in(streams_of[4], 71), 0),
        "row_state": jnp.clip(jnp.exp(math.log(1.0) - 4.6051702 * jax.random.uniform(streams_of[2], (LAY, D), jnp.float32) ** steps_of(streams_of[2], (LAY, D), ((0, 4), (1, 2)), -0.2, 0.2)), 0.01, 1.0),
        "col_state": jnp.clip(jnp.exp(math.log(1.0) - 4.6051702 * jax.random.uniform(streams_of[3], (LAY, QR), jnp.float32) ** steps_of(streams_of[3], (LAY, QR), ((0, 4), (1, 4)), -0.2, 0.2)), 0.01, 1.0),
    }


decay_rate = 0.842
tiny_term = 1e-30
step_share = 0.01
clip_limit = 1.0

def layer_factors(weights, gradient, row_old, col_old):
    grad_float = gradient.astype(jnp.float32)
    squares = grad_float * grad_float + tiny_term
    row_new = decay_rate * row_old + (1.0 - decay_rate) * lax.optimization_barrier(jnp.mean(squares, axis=1))
    col_new = decay_rate * col_old + (1.0 - decay_rate) * lax.optimization_barrier(jnp.mean(squares, axis=0))
    row_norm = row_new / jnp.mean(row_new)
    update = grad_float * lax.rsqrt(row_norm[:, None] * col_new[None, :])
    weight_scale = jnp.sqrt(jnp.mean(weights * weights))
    return (update, weight_scale, row_new, col_new)

def reference(params, grads, row_state, col_state):

    def measure_layer(operands):
        update, weight_scale, row_new, col_new = layer_factors(*operands)
        return (jnp.sum(update * update), weight_scale, row_new, col_new)
    update_sq, weight_scale, row_new, col_new = lax.map(measure_layer, (params, grads, row_state, col_state))
    root_mean = jnp.sqrt(jnp.sum(update_sq) / params.size)
    clip_factor = jnp.maximum(1.0, root_mean / clip_limit)

    def apply_layer(operands):
        weights, gradient, row_old, col_old, layer_scale = operands
        update = layer_factors(weights, gradient, row_old, col_old)[0]
        applied = layer_scale * update / clip_factor
        return (applied, weights - step_share * applied)
    applied_step, new_params = lax.map(apply_layer, (params, grads, row_state, col_state, weight_scale))
    return (new_params, row_new, col_new, applied_step, new_params.astype(jnp.bfloat16))
```

```python
import functools
import jax
import jax.numpy as jnp
from jax import lax
from jax.experimental import pallas as pl
from jax.experimental.pallas import tpu as pltpu
from jax.sharding import PartitionSpec as P

decay_rate = 0.842
tiny_term = 1e-30
step_share = 0.01
clip_limit = 1.0
LANES = 128
f32, bf16 = jnp.float32, jnp.bfloat16


def fold(values):
    return jnp.sum(values.reshape(values.shape[0] // 8, 8, values.shape[1]), axis=0)


def fold_lanes(row):
    return sum(row[:, i : i + LANES] for i in range(0, row.shape[1], LANES))


def split(values):
    high = values.astype(bf16)
    return high, (values - high.astype(f32)).astype(bf16)


def row_dots(left, values):
    dims = (((1,), (1,)), ((), ()))
    high, low = split(values)
    return lax.dot_general(left, high, dims, preferred_element_type=f32) + lax.dot_general(
        left, low, dims, preferred_element_type=f32
    )


def down(row):
    return jnp.broadcast_to(row, (LANES, LANES)).T


def exchange(axis, pick, send, recv, base=0):
    n, me = lax.axis_size(axis), lax.axis_index(axis)
    copies = []
    for d in range(1, n):
        copy = pltpu.make_async_remote_copy(
            src_ref=pick(me),
            dst_ref=pick(me),
            send_sem=send.at[base + d - 1],
            recv_sem=recv.at[base + d - 1],
            device_id={axis: lax.rem(me + d, n)},
            device_id_type=pl.DeviceIdType.MESH,
        )
        copy.start()
        copies.append(copy)
    return copies


def finish(copies):
    for copy in copies:
        copy.wait()


def total(parts):
    return functools.reduce(lambda a, b: a + b, parts)


def loop(low, high, step):
    def one(k, carry):
        step(k)
        return carry

    lax.fori_loop(low, high, one, 0)


def step_kernel(
    layers, per, late,
    p_hbm, g_hbm, row_ref, col_ref,
    row_out, col_out, root_out, step_out, all_hbm, late_hbm,
    p_vm, g_vm, new_vm, row_all, col_all, mean_all, up_z, up_y, up_x, old_row, new_row, inverse,
    p_sem, g_sem, o_sem,
    rz_s, rz_r, cy_s, cy_r, my_s, my_r, uz_s, uz_r, uy_s, uy_r, ux_s, ux_r,
    right_s, right_r, left_s, left_r,
):
    flat, columns = g_vm.shape
    rows = flat // layers
    nb, chunk = rows // LANES, per * LANES
    chunks = nb // per
    count = layers * chunks
    nx, ny, nz = (lax.axis_size(a) for a in ("gx", "gy", "gz"))
    me_x, me_y, me_z = (lax.axis_index(a) for a in ("gx", "gy", "gz"))
    rows_all, columns_all = rows * ny, columns * nz

    def part(k):
        return pl.ds(pl.multiple_of(k * chunk, chunk), chunk)

    def block(b):
        return pl.ds(pl.multiple_of(b * LANES, LANES), LANES)

    def g_load(k):
        return pltpu.make_async_copy(g_hbm.at[part(k)], g_vm.at[part(k)], g_sem.at[k])

    def p_load(k):
        return pltpu.make_async_copy(p_hbm.at[part(k)], p_vm.at[part(k)], p_sem.at[k])

    loop(0, count, lambda k: g_load(k).start())
    loop(0, count, lambda k: p_load(k).start())

    barrier = pltpu.get_barrier_semaphore()
    for axis, n, me in (("gx", nx, me_x), ("gy", ny, me_y), ("gz", nz, me_z)):
        for d in range(1, n):
            pl.semaphore_signal(
                barrier, inc=1, device_id={axis: lax.rem(me + d, n)},
                device_id_type=pl.DeviceIdType.MESH,
            )

    for l in range(layers):
        for b in range(nb):
            old_row[l, b : b + 1, :] = row_ref[l : l + 1, b * LANES : (b + 1) * LANES]
        if row_all.shape[2] > nb:
            row_all[me_z, l, nb:, :] = jnp.zeros((row_all.shape[2] - nb, LANES), f32)
    up_z[me_z] = jnp.zeros(up_z.shape[1:], f32)
    pl.semaphore_wait(barrier, nx + ny + nz - 3)

    ones = jnp.ones((16, LANES), bf16)
    first = []
    for l in range(layers):

        def measure_chunk(c, col_sum, l=l):
            k = l * chunks + c
            g_load(k).wait()

            def measure(b, col_sum):
                grad = g_vm[block(k * per + b), :].astype(f32)
                squares = grad * grad
                row_all[me_z, l, pl.ds(c * per + b, 1), :] = row_dots(ones, fold_lanes(squares))[0:1]
                return col_sum + fold(squares)

            return lax.fori_loop(0, per, measure, col_sum, unroll=True)

        col_all[me_y, l] = lax.fori_loop(0, chunks, measure_chunk, jnp.zeros((8, columns), f32))
        first.append(
            exchange("gz", lambda me, l=l: row_all.at[me, l], rz_s, rz_r, l * (nz - 1))
            + exchange("gy", lambda me, l=l: col_all.at[me, l], cy_s, cy_r, l * (ny - 1))
        )

    def weigh_params(l):
        def weigh_chunk(c, acc):
            k = l * chunks + c
            p_load(k).wait()

            def one(b, acc):
                weights = p_vm[block(k * per + b), :]
                return acc + fold(fold_lanes(weights * weights))

            return lax.fori_loop(0, per, one, acc, unroll=True)

        acc = lax.fori_loop(0, chunks, weigh_chunk, jnp.zeros((8, LANES), f32))
        up_z[me_z, 1 + l : 2 + l, :] = jnp.sum(acc, axis=0, keepdims=True)

    for l in range(layers - 1):
        weigh_params(l)

    means, lane_sums = [], []
    for l in range(layers):
        finish(first[l])
        row_mean_sq = total([row_all[z, l, 0:nb, :] for z in range(nz)]) / columns_all + tiny_term
        row_now = decay_rate * old_row[l, 0:nb, :] + (1.0 - decay_rate) * row_mean_sq
        new_row[l, 0:nb, :] = row_now
        inverse[l, 0:nb, :] = 1.0 / row_now
        mean_all[me_y, l] = jnp.broadcast_to(jnp.sum(row_now, axis=0, keepdims=True), (8, LANES))
        means += exchange("gy", lambda me, l=l: mean_all.at[me, l], my_s, my_r, l * (ny - 1))
        col_sum = jnp.sum(total([col_all[y, l] for y in range(ny)]), axis=0, keepdims=True)
        col_now = decay_rate * col_ref[l : l + 1, :] + (1.0 - decay_rate) * (
            col_sum / rows_all + tiny_term
        )
        col_out[l : l + 1, :] = col_now
        inverse_col = 1.0 / col_now

        def weigh_chunk(c, acc, l=l, inverse_col=inverse_col):
            def weigh(b, acc):
                grad = g_vm[block((l * chunks + c) * per + b), :].astype(f32)
                share = fold_lanes(grad * grad * inverse_col)
                return acc + fold(share * down(inverse[l, pl.ds(c * per + b, 1), :]))

            return lax.fori_loop(0, per, weigh, acc, unroll=True)

        lane_sums.append(lax.fori_loop(0, chunks, weigh_chunk, jnp.zeros((8, LANES), f32)))

    weigh_params(layers - 1)
    finish(means)
    row_means = []
    for l in range(layers):
        row_sum = total([mean_all[y, l, 0:1, :] for y in range(ny)])
        row_means.append(jnp.sum(row_sum, axis=1, keepdims=True) / rows_all)
    up_z[me_z, 0:1, :] = total(
        [jnp.sum(lane_sums[l], axis=0, keepdims=True) * row_means[l] for l in range(layers)]
    )

    copies = exchange("gz", lambda me: up_z.at[me], uz_s, uz_r)
    for l in range(layers):
        inverse[l, 0:nb, :] = lax.rsqrt(new_row[l, 0:nb, :] / row_means[l])
    finish(copies)
    up_y[me_y] = total([up_z[z] for z in range(nz)])
    finish(exchange("gy", lambda me: up_y.at[me], uy_s, uy_r))
    up_x[me_x] = total([up_y[y] for y in range(ny)])
    copies = exchange("gx", lambda me: up_x.at[me], ux_s, ux_r)
    weight_sums = jnp.sum(up_x[me_x, 1 : 1 + layers, :], axis=1, keepdims=True)
    scaled = lax.rsqrt(col_out[...]) * jnp.sqrt(weight_sums / (rows_all * columns_all))
    finish(copies)
    update_total = jnp.sum(total([up_x[x, 0:1, :] for x in range(nx)]), axis=1, keepdims=True)
    entries = layers * nx * rows_all * columns_all
    clip_factor = jnp.maximum(1.0, jnp.sqrt(update_total / entries) / clip_limit)
    col_step = scaled / clip_factor
    step_out[...] = col_step

    sides = ((1, me_z, right_s, right_r), (-1, nz - 1 - me_z, left_s, left_r))

    def late_part(k):
        return pl.ds(pl.multiple_of((k - (count - late)) * chunk, chunk), chunk)

    def hop(side, s, k, to_late=False):
        way, _, send, recv = side
        shard = me_z - way * (s - 1)
        slot = (s - 1) * count + k
        target = late_hbm.at[late_part(k)] if to_late else all_hbm.at[shard, part(k)]
        return pltpu.make_async_remote_copy(
            src_ref=new_vm.at[part(k)] if s == 1 else all_hbm.at[shard, part(k)],
            dst_ref=target,
            send_sem=send.at[slot],
            recv_sem=recv.at[slot],
            device_id={"gz": me_z + way},
            device_id_type=pl.DeviceIdType.MESH,
        )

    def arrival(side, s, k):
        way, _, send, recv = side
        slot = (s - 1) * count + k
        here = all_hbm.at[me_z - way * s, part(k)]
        return pltpu.make_async_remote_copy(
            src_ref=here,
            dst_ref=here,
            send_sem=send.at[slot],
            recv_sem=recv.at[slot],
            device_id={"gz": me_z + way},
            device_id_type=pl.DeviceIdType.MESH,
        )

    def for_hop(side, s, k, is_late, act):
        place = side[1]
        if s == nz - 1 and is_late:
            return
        if s == nz - 2 and is_late:

            @pl.when(place == nz - 3)
            def _():
                act(hop(side, s, k, True))

            @pl.when(place == nz - 2)
            def _():
                act(hop(side, s, k))

        else:

            @pl.when(jnp.logical_and(place >= s - 1, place < nz - 1))
            def _():
                act(hop(side, s, k))

    def own(k):
        return pltpu.make_async_copy(new_vm.at[part(k)], all_hbm.at[me_z, part(k)], o_sem.at[k])

    def launch(k):
        for side in sides:
            for_hop(side, 1, k, False, lambda copy: copy.start())
        own(k).start()

    less = col_step * step_share
    for l in range(layers):

        def apply_chunk(c, l=l):
            k = l * chunks + c

            def apply(b, carry):
                here = block(k * per + b)
                root = down(inverse[l, pl.ds(c * per + b, 1), :])
                for j in range(0, columns, LANES):
                    cut = slice(j, j + LANES)
                    taken = g_vm[here, cut].astype(f32) * root * less[l : l + 1, cut]
                    new_vm[here, cut] = (p_vm[here, cut] - taken).astype(bf16)
                return carry

            lax.fori_loop(0, per, apply, 0, unroll=True)
            pl.when(k > 0)(lambda: launch(k - 1))

        loop(0, chunks, apply_chunk)
    launch(count - 1)

    for l in range(layers):
        for b in range(nb):
            cut = slice(b * LANES, (b + 1) * LANES)
            row_out[l : l + 1, cut] = new_row[l, b : b + 1, :]
            root_out[l : l + 1, cut] = inverse[l, b : b + 1, :]

    for s in range(1, nz):
        for low, high, is_late in ((0, count - late, False), (count - late, count, True)):
            if s == nz - 1 and is_late:
                continue

            def pass_on(k, s=s, is_late=is_late):
                for side in sides:
                    pl.when(side[1] >= s)(lambda side=side: arrival(side, s, k).wait_recv())
                    if s + 1 < nz:
                        for_hop(side, s + 1, k, is_late, lambda copy: copy.start())

            loop(low, high, pass_on)

    for s in range(1, nz):
        for low, high, is_late in ((0, count - late, False), (count - late, count, True)):

            def sent(k, s=s, is_late=is_late):
                for side in sides:
                    for_hop(side, s, k, is_late, lambda copy: copy.wait_send())

            loop(low, high, sent)
    loop(0, count, lambda k: own(k).wait())


def cuts(layers, rows):
    nb = rows // LANES
    per = max(q for q in range(1, 9) if nb % q == 0)
    count = layers * (nb // per)
    return per, count, max(1, count // 3)


def step(params, grads, row_state, col_state):
    layers, rows, columns = params.shape
    nx, ny, nz = (lax.axis_size(a) for a in ("gx", "gy", "gz"))
    assert nz > 3
    flat = layers * rows
    nb = rows // LANES
    per, count, late = cuts(layers, rows)
    padded = -(-nb // 8) * 8
    tall = -(-(1 + layers) // 8) * 8
    sem = lambda n: pltpu.SemaphoreType.DMA((max(n, 1),))
    vmem, anywhere = pl.BlockSpec(memory_space=pltpu.VMEM), pl.BlockSpec(memory_space=pl.ANY)
    pairs = [layers * (nz - 1), layers * (ny - 1), layers * (ny - 1), nz - 1, ny - 1, nx - 1]
    pairs += [(nz - 1) * count] * 2
    return pl.pallas_call(
        functools.partial(step_kernel, layers, per, late),
        out_shape=(
            jax.ShapeDtypeStruct((layers, rows), f32),
            jax.ShapeDtypeStruct((layers, columns), f32),
            jax.ShapeDtypeStruct((layers, rows), f32),
            jax.ShapeDtypeStruct((layers, columns), f32),
            jax.ShapeDtypeStruct((nz, flat, columns), bf16),
            jax.ShapeDtypeStruct((late * per * LANES, columns), bf16),
        ),
        in_specs=[anywhere, anywhere, vmem, vmem],
        out_specs=(vmem, vmem, vmem, vmem, anywhere, anywhere),
        scratch_shapes=[
            pltpu.VMEM((flat, columns), f32),
            pltpu.VMEM((flat, columns), bf16),
            pltpu.VMEM((flat, columns), bf16),
            pltpu.VMEM((nz, layers, padded, LANES), f32),
            pltpu.VMEM((ny, layers, 8, columns), f32),
            pltpu.VMEM((ny, layers, 8, LANES), f32),
            pltpu.VMEM((nz, tall, LANES), f32),
            pltpu.VMEM((ny, tall, LANES), f32),
            pltpu.VMEM((nx, tall, LANES), f32),
            pltpu.VMEM((layers, padded, LANES), f32),
            pltpu.VMEM((layers, padded, LANES), f32),
            pltpu.VMEM((layers, padded, LANES), f32),
            sem(count),
            sem(count),
            sem(count),
        ]
        + [sem(n) for n in pairs for _ in range(2)],
        compiler_params=pltpu.CompilerParams(
            collective_id=0, has_side_effects=True, vmem_limit_bytes=60 * 1024 * 1024
        ),
        cost_estimate=pl.CostEstimate(
            flops=20 * flat * columns, bytes_accessed=8 * flat * columns, transcendentals=0
        ),
    )(params.reshape(flat, columns), grads.reshape(flat, columns), row_state, col_state)


def place_kernel(late_chunks, chunk, from_hbm, out_hbm, stage, in_sem, out_sem):
    n, flat, columns = from_hbm.shape
    count, me = flat // chunk, lax.axis_index("gz")

    def copies(d, k):
        part = pl.ds(pl.multiple_of(k * chunk, chunk), chunk)
        slot = d * count + k
        return (
            pltpu.make_async_copy(from_hbm.at[d, part], stage.at[d, part], in_sem.at[slot]),
            pltpu.make_async_copy(
                stage.at[d, part], out_hbm.at[part, pl.ds(d * columns, columns)], out_sem.at[slot]
            ),
        )

    def whole(act):
        for d in range(n):
            missing = me < 2 if d == n - 1 else me > n - 3 if d == 0 else None
            loop(0, count - late_chunks, lambda k, d=d: act(*copies(d, k)))
            rest = lambda d=d: loop(count - late_chunks, count, lambda k: act(*copies(d, k)))
            if missing is None:
                rest()
            else:
                pl.when(jnp.logical_not(missing))(rest)

    def relay(take, put):
        take.wait()
        put.start()

    whole(lambda take, put: take.start())
    whole(relay)
    whole(lambda take, put: put.wait())


def place(gathered, late_chunks, chunk):
    n, flat, columns = gathered.shape
    anywhere = pl.BlockSpec(memory_space=pl.ANY)
    slots = n * (flat // chunk)
    return pl.pallas_call(
        functools.partial(place_kernel, late_chunks, chunk),
        in_specs=[anywhere],
        out_specs=anywhere,
        out_shape=jax.ShapeDtypeStruct((flat, n * columns), bf16),
        scratch_shapes=[
            pltpu.VMEM((n, flat, columns), bf16),
            pltpu.SemaphoreType.DMA((slots,)),
            pltpu.SemaphoreType.DMA((slots,)),
        ],
        compiler_params=pltpu.CompilerParams(vmem_limit_bytes=60 * 1024 * 1024),
        cost_estimate=pl.CostEstimate(
            flops=n * flat * columns, bytes_accessed=4 * n * flat * columns, transcendentals=0
        ),
    )(gathered)


def place_late_kernel(n, chunk, held_hbm, late_hbm, moved_hbm, out_hbm, stage, in_sem, out_sem):
    rows, columns = late_hbm.shape
    count, me = rows // chunk, lax.axis_index("gz")
    start = out_hbm.shape[0] - rows

    def move(source, d):
        def copies(k):
            part = pl.ds(k * chunk, chunk)
            there = pl.ds(start + k * chunk, chunk)
            return (
                pltpu.make_async_copy(source.at[part], stage.at[part], in_sem.at[k]),
                pltpu.make_async_copy(
                    stage.at[part], out_hbm.at[there, pl.ds(d * columns, columns)], out_sem.at[k]
                ),
            )

        both = [copies(k) for k in range(count)]
        for take, _ in both:
            take.start()
        for take, put in both:
            take.wait()
            put.start()
        for _, put in both:
            put.wait()

    for at, source, d in (
        (0, moved_hbm, n - 1), (1, late_hbm, n - 1), (n - 2, late_hbm, 0), (n - 1, moved_hbm, 0)
    ):
        pl.when(me == at)(lambda source=source, d=d: move(source, d))


def place_late(held, late, moved, n, chunk):
    anywhere = pl.BlockSpec(memory_space=pl.ANY)
    rows, columns = late.shape
    return pl.pallas_call(
        functools.partial(place_late_kernel, n, chunk),
        in_specs=[anywhere] * 3,
        out_specs=anywhere,
        out_shape=jax.ShapeDtypeStruct(held.shape, bf16),
        scratch_shapes=[
            pltpu.VMEM((rows, columns), bf16),
            pltpu.SemaphoreType.DMA((rows // chunk,)),
            pltpu.SemaphoreType.DMA((rows // chunk,)),
        ],
        input_output_aliases={0: 0},
        cost_estimate=pl.CostEstimate(
            flops=rows * columns, bytes_accessed=4 * rows * columns, transcendentals=0
        ),
    )(held, late, moved)


def body(params, grads, row_state, col_state):
    layers, rows, columns = params.shape
    n = lax.axis_size("gz")
    per, count, late_chunks = cuts(layers, rows)
    row_new, col_new, row_root, col_step, gathered, late = step(
        params, grads, row_state, col_state
    )
    moved = lax.ppermute(late, "gz", [(n - 2, n - 1), (1, 0)])
    applied = grads.astype(f32) * row_root[:, :, None] * col_step[:, None, :]
    new_params = params - step_share * applied
    held = place(gathered, late_chunks, per * LANES)
    held = place_late(held, late, moved, n, per * LANES)
    compute = held.reshape(layers, rows, n * columns)
    return (new_params, row_new, col_new, applied, compute)


def solution(mesh):
    in_specs = (P("gx", "gy", "gz"), P("gx", "gy", "gz"), P("gx", "gy"), P("gx", "gz"))
    out_specs = (
        P("gx", "gy", "gz"),
        P("gx", "gy"),
        P("gx", "gz"),
        P("gx", "gy", "gz"),
        P("gx", "gy", None),
    )
    return jax.shard_map(body, mesh=mesh, in_specs=in_specs, out_specs=out_specs, check_vma=False)
```

```python
import functools
import itertools
import jax
import jax.numpy as jnp
from jax import lax
from jax.experimental import pallas as pl
from jax.experimental.pallas import tpu as pltpu
from jax.sharding import PartitionSpec as P

decay_rate = 0.842
tiny_term = 1e-30
step_share = 0.01
clip_limit = 1.0
LANES = 128
f32, bf16 = jnp.float32, jnp.bfloat16


def fold(values):
    return jnp.sum(values.reshape(values.shape[0] // 8, 8, values.shape[1]), axis=0)


def fold_lanes(row):
    return sum(row[:, i : i + LANES] for i in range(0, row.shape[1], LANES))


def down(row):
    return jnp.broadcast_to(row, (LANES, LANES)).T


def peers(axes):
    mine = [lax.axis_index(a) for a in axes]
    sizes = [lax.axis_size(a) for a in axes]
    for shift in itertools.product(*[range(n) for n in sizes]):
        if any(shift):
            yield {a: lax.rem(m + d, n) for a, m, d, n in zip(axes, mine, shift, sizes)}


def exchange(axes, mine, send, recv, base, act):
    for slot, device in enumerate(peers(axes)):
        act(
            pltpu.make_async_remote_copy(
                src_ref=mine,
                dst_ref=mine,
                send_sem=send.at[base + slot],
                recv_sem=recv.at[base + slot],
                device_id=device,
                device_id_type=pl.DeviceIdType.MESH,
            )
        )


def start(copy):
    copy.start()


def finish(copy):
    copy.wait()


def total(parts):
    return functools.reduce(lambda a, b: a + b, parts)


def loop(low, high, step):
    def one(k, carry):
        step(k)
        return carry

    lax.fori_loop(low, high, one, 0)


def step_kernel(
    layers, per, late, early,
    p_hbm, g_hbm, row_hbm, col_hbm,
    row_out, col_out, root_out, step_out, all_hbm, late_hbm,
    p_vm, g_vm, new_vm, row_vm, root_vm, old_col, col_vm, step_vm,
    row_all, col_all, sum_all, up_all, new_row, inverse, root,
    near_p, near_g, near_col, near_new,
    p_sem, g_sem, o_sem, small_in, small_out, near_s, near_r, near_o,
    rz_s, rz_r, cy_s, cy_r, sum_s, sum_r, up_s, up_r,
    right_s, right_r, left_s, left_r,
):
    flat, columns = g_vm.shape
    rows = flat // layers
    nb, chunk = rows // LANES, per * LANES
    chunks = nb // per
    count = layers * chunks
    nx, ny, nz = (lax.axis_size(a) for a in ("gx", "gy", "gz"))
    me_x, me_y, me_z = (lax.axis_index(a) for a in ("gx", "gy", "gz"))
    rows_all, columns_all = rows * ny, columns * nz

    def part(k):
        return pl.ds(pl.multiple_of(k * chunk, chunk), chunk)

    def block(b):
        return pl.ds(pl.multiple_of(b * LANES, LANES), LANES)

    def g_load(k):
        return pltpu.make_async_copy(g_hbm.at[part(k)], g_vm.at[part(k)], g_sem.at[k])

    def p_load(k):
        return pltpu.make_async_copy(p_hbm.at[part(k)], p_vm.at[part(k)], p_sem.at[k])

    sides = ((1, me_z, right_s, right_r), (-1, nz - 1 - me_z, left_s, left_r))

    loop(0, count, lambda k: g_load(k).start())
    olds = [
        pltpu.make_async_copy(row_hbm, row_vm, small_in.at[0]),
        pltpu.make_async_copy(col_hbm, old_col, small_in.at[1]),
    ]
    for copy in olds:
        copy.start()
    loop(0, count, lambda k: p_load(k).start())

    plane = ("gy", "gz")
    barrier = pltpu.get_barrier_semaphore()
    for device in itertools.chain(peers(plane), peers(("gx",))):
        pl.semaphore_signal(
            barrier, inc=1, device_id=device, device_id_type=pl.DeviceIdType.MESH
        )

    if per < 8:

        def clear(k):
            row_all[me_z, k, per:, :] = jnp.zeros((8 - per, LANES), f32)

        loop(0, count, clear)

    def rows_of(k, act):
        exchange(("gz",), row_all.at[me_z, k], rz_s, rz_r, k * (nz - 1), act)

    def columns_of(l, act):
        exchange(("gy",), col_all.at[me_y, l], cy_s, cy_r, l * (ny - 1), act)

    for l in range(layers):

        def measure_chunk(c, col_sum, l=l):
            k = l * chunks + c
            g_load(k).wait()
            for b in range(per):
                grad = g_vm[block(k * per + b), :].astype(f32)
                squares = grad * grad
                row_all[me_z, k, b : b + 1, :] = jnp.sum(
                    fold_lanes(squares).T, axis=0, keepdims=True
                )
                col_sum = col_sum + fold(squares)
            if l > 0:
                rows_of(k, start)
            return col_sum

        col_all[me_y, l] = lax.fori_loop(0, chunks, measure_chunk, jnp.zeros((8, columns), f32))
        if l == 0:
            pl.semaphore_wait(barrier, ny * nz + nx - 2)
            loop(0, chunks, lambda c: rows_of(c, start))
        columns_of(l, start)

    for copy in olds:
        copy.wait()
    for l in range(layers):
        for b in range(nb):
            new_row[l * chunks + b // per, b % per : b % per + 1, :] = row_vm[
                l : l + 1, b * LANES : (b + 1) * LANES
            ]

    packed = jnp.zeros((2, LANES), f32)
    lane = lax.broadcasted_iota(jnp.int32, (2, LANES), 1)
    line = lax.broadcasted_iota(jnp.int32, (2, LANES), 0)

    def pack(packed, at_line, at_lane, values):
        value = jnp.sum(jnp.sum(values, axis=0, keepdims=True), axis=1, keepdims=True)
        return jnp.where(jnp.logical_and(line == at_line, lane == at_lane), value, packed)

    for l in range(layers):

        def params_chunk(c, acc, l=l):
            k = l * chunks + c
            p_load(k).wait()
            for b in range(per):
                weights = p_vm[block(k * per + b), :]
                acc = acc + fold(fold_lanes(weights * weights))
            return acc

        params_sum = lax.fori_loop(0, chunks, params_chunk, jnp.zeros((8, LANES), f32))

        columns_of(l, finish)
        col_sum = jnp.sum(total([col_all[y, l] for y in range(ny)]), axis=0, keepdims=True)
        col_now = decay_rate * old_col[l : l + 1, :] + (1.0 - decay_rate) * (
            col_sum / rows_all + tiny_term
        )
        col_vm[l : l + 1, :] = col_now
        inverse_col = 1.0 / col_now

        def weigh_chunk(c, carry, l=l, inverse_col=inverse_col):
            acc, row_sum = carry
            k = l * chunks + c
            rows_of(k, finish)
            squares = total([row_all[z, k, 0:per, :] for z in range(nz)]) / columns_all + tiny_term
            row_now = decay_rate * new_row[k, 0:per, :] + (1.0 - decay_rate) * squares
            new_row[k, 0:per, :] = row_now
            inverse[k, 0:per, :] = 1.0 / row_now
            root[k, 0:per, :] = lax.rsqrt(row_now)
            for b in range(per):
                grad = g_vm[block(k * per + b), :].astype(f32)
                share = fold_lanes(grad * grad * inverse_col)
                acc = acc + fold(share * down(inverse[k, b : b + 1, :]))
            return acc, row_sum + row_now

        acc, row_sum = lax.fori_loop(
            0, chunks, weigh_chunk, (jnp.zeros((8, LANES), f32), jnp.zeros((per, LANES), f32))
        )
        packed = pack(packed, 0, l, acc)
        packed = pack(packed, 1, l, row_sum)
        packed = pack(packed, 0, layers + l, params_sum)

    sum_all[me_y, me_z] = packed
    exchange(plane, sum_all.at[me_y, me_z], sum_s, sum_r, 0, start)

    last = pl.ds(flat - early, early)

    def near(side, act):
        for i, (source, target) in enumerate(
            ((col_vm, near_col), (p_hbm.at[last], near_p), (g_hbm.at[last], near_g))
        ):
            act(
                pltpu.make_async_remote_copy(
                    src_ref=source,
                    dst_ref=target,
                    send_sem=near_s.at[i],
                    recv_sem=near_r.at[i],
                    device_id={"gz": me_z + side[0]},
                    device_id_type=pl.DeviceIdType.MESH,
                )
            )

    for side in sides:
        pl.when(side[1] == nz - 2)(lambda side=side: near(side, start))
    col_root = lax.rsqrt(col_vm[...])
    exchange(plane, sum_all.at[me_y, me_z], sum_s, sum_r, 0, finish)
    here = total([sum_all[y, z] for y in range(ny) for z in range(nz)])
    both = jnp.where(lane[0:1] < layers, here[0:1] * here[1:2], 0.0)
    up_all[me_x] = jnp.broadcast_to(both, (2, LANES))
    exchange(("gx",), up_all.at[me_x], up_s, up_r, 0, start)
    parts, scales = [], []
    for l in range(layers):
        row_mean = here[1:2, l : l + 1] / (nz * rows_all)
        weight_scale = jnp.sqrt(here[0:1, layers + l : layers + l + 1] / (rows_all * columns_all))
        scales.append(jnp.sqrt(row_mean) * weight_scale)
        parts.append(col_root[l : l + 1] * scales[l])
    exchange(("gx",), up_all.at[me_x], up_s, up_r, 0, finish)
    update_sum = total([up_all[x, 0:1] for x in range(nx)])
    update_total = jnp.sum(update_sum, axis=1, keepdims=True) / (nz * rows_all)
    entries = layers * nx * rows_all * columns_all
    clip_factor = jnp.maximum(1.0, jnp.sqrt(update_total / entries) / clip_limit)
    for l in range(layers):
        step_vm[l : l + 1, :] = parts[l] / clip_factor
    less = step_vm[...] * step_share

    def late_part(k):
        return pl.ds(pl.multiple_of((k - (count - late)) * chunk, chunk), chunk)

    def size_of(k, short):
        return pl.ds(pl.multiple_of(k * chunk, chunk), chunk - early) if short else part(k)

    def hop(side, s, k, to_late=False, short=False):
        way, _, send, recv = side
        shard = me_z - way * (s - 1)
        slot = (s - 1) * count + k
        rows_k = size_of(k, short)
        target = late_hbm.at[late_part(k)] if to_late else all_hbm.at[shard, rows_k]
        return pltpu.make_async_remote_copy(
            src_ref=new_vm.at[rows_k] if s == 1 else all_hbm.at[shard, rows_k],
            dst_ref=target,
            send_sem=send.at[slot],
            recv_sem=recv.at[slot],
            device_id={"gz": me_z + way},
            device_id_type=pl.DeviceIdType.MESH,
        )

    def arrival(side, s, k, short=False):
        way, _, send, recv = side
        slot = (s - 1) * count + k
        here = all_hbm.at[me_z - way * s, size_of(k, short)]
        return pltpu.make_async_remote_copy(
            src_ref=here,
            dst_ref=here,
            send_sem=send.at[slot],
            recv_sem=recv.at[slot],
            device_id={"gz": me_z + way},
            device_id_type=pl.DeviceIdType.MESH,
        )

    def for_arrival(side, s, k, final):
        if final:
            pl.when(side[1] == nz - 1)(lambda: arrival(side, s, k, True).wait_recv())
            full = jnp.logical_and(side[1] >= s, side[1] < nz - 1)
        else:
            full = side[1] >= s
        pl.when(full)(lambda: arrival(side, s, k).wait_recv())

    def for_hop(side, s, k, is_late, act, final=False):
        place = side[1]
        if s == nz - 1 and is_late:
            return
        if s == nz - 2 and is_late:

            @pl.when(place == nz - 3)
            def _():
                act(hop(side, s, k, True))

            @pl.when(place == nz - 2)
            def _():
                act(hop(side, s, k))

        elif final:

            @pl.when(place < nz - 2)
            def _():
                act(hop(side, s, k))

            @pl.when(place == nz - 2)
            def _():
                act(hop(side, s, k, short=True))

        else:

            @pl.when(jnp.logical_and(place >= s - 1, place < nz - 1))
            def _():
                act(hop(side, s, k))

    def own(k):
        return pltpu.make_async_copy(new_vm.at[part(k)], all_hbm.at[me_z, part(k)], o_sem.at[k])

    def launch(k, final=False):
        for side in sides:
            for_hop(side, 1, k, False, start, final)
        own(k).start()

    for l in range(layers):

        def apply_chunk(c, l=l):
            k = l * chunks + c

            for b in range(per):
                here = block(k * per + b)
                factor = down(root[k, b : b + 1, :])
                for j in range(0, columns, LANES):
                    cut = slice(j, j + LANES)
                    taken = g_vm[here, cut].astype(f32) * factor * less[l : l + 1, cut]
                    new_vm[here, cut] = (p_vm[here, cut] - taken).astype(bf16)

            pl.when(k > 0)(lambda: launch(k - 1))

        loop(0, chunks, apply_chunk)
    launch(count - 1, True)

    def near_rows(side):
        near(side, lambda copy: copy.wait_recv())
        l, k = layers - 1, count - 1
        near_less = lax.rsqrt(near_col[l : l + 1, :]) * scales[l] / clip_factor * step_share
        skip = chunk - early
        for b in range(skip // LANES, per):
            low = max(0, skip - b * LANES)
            rows_b = slice(b * LANES + low - skip, (b + 1) * LANES - skip)
            factor = down(root[k, b : b + 1, :])[low:, :]
            for j in range(0, columns, LANES):
                cut = slice(j, j + LANES)
                taken = near_g[rows_b, cut].astype(f32) * factor * near_less[:, cut]
                near_new[rows_b, cut] = (near_p[rows_b, cut] - taken).astype(bf16)

    def near_put(side):
        return pltpu.make_async_copy(near_new, all_hbm.at[me_z - side[0], last], near_o)

    for side in sides:
        pl.when(side[1] == nz - 1)(lambda side=side: near_rows(side))
        pl.when(side[1] == nz - 2)(lambda side=side: near(side, lambda copy: copy.wait_send()))

    for l in range(layers):
        for b in range(nb):
            cut = slice(b * LANES, (b + 1) * LANES)
            k, i = l * chunks + b // per, b % per
            row_vm[l : l + 1, cut] = new_row[k, i : i + 1, :]
            root_vm[l : l + 1, cut] = root[k, i : i + 1, :]
    smalls = [
        pltpu.make_async_copy(source, target, small_out.at[i])
        for i, (source, target) in enumerate(
            ((row_vm, row_out), (col_vm, col_out), (root_vm, root_out), (step_vm, step_out))
        )
    ]
    for copy in smalls:
        copy.start()

    for side in sides:
        pl.when(side[1] == nz - 1)(lambda side=side: near_put(side).start())

    def pass_on(s, k, is_late, final=False):
        for side in sides:
            for_arrival(side, s, k, final)
            if s + 1 < nz:
                for_hop(side, s + 1, k, is_late, start)
        for side in sides:
            for_hop(side, s, k, is_late, lambda copy: copy.wait_send(), final)

    for s in range(1, nz):
        if s == nz - 1:
            loop(0, count, lambda k: own(k).wait())
            for copy in smalls:
                copy.wait()
            for side in sides:
                pl.when(side[1] == nz - 1)(lambda side=side: near_put(side).wait())
        loop(0, count - late, lambda k, s=s: pass_on(s, k, False))
        if s == 1:
            loop(count - late, count - 1, lambda k: pass_on(1, k, True))
            pass_on(1, count - 1, True, True)
        elif s < nz - 1:
            loop(count - late, count, lambda k, s=s: pass_on(s, k, True))


def cuts(layers, rows):
    nb = rows // LANES
    per = max(q for q in range(1, 9) if nb % q == 0)
    count = layers * (nb // per)
    return per, count, max(1, count // 3), min(192, (per - 1) * LANES)


def step(params, grads, row_state, col_state):
    layers, rows, columns = params.shape
    nx, ny, nz = (lax.axis_size(a) for a in ("gx", "gy", "gz"))
    assert nz > 3
    flat = layers * rows
    per, count, late, early = cuts(layers, rows)
    sem = lambda n: pltpu.SemaphoreType.DMA((max(n, 1),))
    anywhere = pl.BlockSpec(memory_space=pl.ANY)
    pairs = [count * (nz - 1), layers * (ny - 1), ny * nz - 1, nx - 1] + [(nz - 1) * count] * 2
    return pl.pallas_call(
        functools.partial(step_kernel, layers, per, late, early),
        out_shape=(
            jax.ShapeDtypeStruct((layers, rows), f32),
            jax.ShapeDtypeStruct((layers, columns), f32),
            jax.ShapeDtypeStruct((layers, rows), f32),
            jax.ShapeDtypeStruct((layers, columns), f32),
            jax.ShapeDtypeStruct((nz, flat, columns), bf16),
            jax.ShapeDtypeStruct((late * per * LANES, columns), bf16),
        ),
        in_specs=[anywhere] * 4,
        out_specs=(anywhere,) * 6,
        scratch_shapes=[
            pltpu.VMEM((flat, columns), f32),
            pltpu.VMEM((flat, columns), bf16),
            pltpu.VMEM((flat, columns), bf16),
            pltpu.VMEM((layers, rows), f32),
            pltpu.VMEM((layers, rows), f32),
            pltpu.VMEM((layers, columns), f32),
            pltpu.VMEM((layers, columns), f32),
            pltpu.VMEM((layers, columns), f32),
            pltpu.VMEM((nz, count, 8, LANES), f32),
            pltpu.VMEM((ny, layers, 8, columns), f32),
            pltpu.VMEM((ny, nz, 2, LANES), f32),
            pltpu.VMEM((nx, 2, LANES), f32),
            pltpu.VMEM((count, 8, LANES), f32),
            pltpu.VMEM((count, 8, LANES), f32),
            pltpu.VMEM((count, 8, LANES), f32),
            pltpu.VMEM((early, columns), f32),
            pltpu.VMEM((early, columns), bf16),
            pltpu.VMEM((layers, columns), f32),
            pltpu.VMEM((early, columns), bf16),
            sem(count),
            sem(count),
            sem(count),
            sem(2),
            sem(4),
            sem(3),
            sem(3),
            pltpu.SemaphoreType.DMA,
        ]
        + [sem(n) for n in pairs for _ in range(2)],
        compiler_params=pltpu.CompilerParams(
            collective_id=0, has_side_effects=True, vmem_limit_bytes=60 * 1024 * 1024
        ),
        cost_estimate=pl.CostEstimate(
            flops=20 * flat * columns, bytes_accessed=8 * flat * columns, transcendentals=0
        ),
    )(params.reshape(flat, columns), grads.reshape(flat, columns), row_state, col_state)


def place_kernel(
    late_chunks, chunk, from_hbm, late_hbm, row_in, col_in,
    out_hbm, row_out, col_out, stage, in_sem, out_sem,
):
    n, flat, columns = from_hbm.shape
    count, me = flat // chunk, lax.axis_index("gz")
    main = count - late_chunks
    row_out[...] = row_in[...]
    col_out[...] = col_in[...]

    def part(k):
        return pl.ds(pl.multiple_of(k * chunk, chunk), chunk)

    def copies(d, k, source):
        slot = d * count + k
        return (
            pltpu.make_async_copy(source, stage.at[d, part(k)], in_sem.at[slot]),
            pltpu.make_async_copy(
                stage.at[d, part(k)],
                out_hbm.at[part(k), pl.ds(d * columns, columns)],
                out_sem.at[slot],
            ),
        )

    def whole(act):
        for d in range(n):
            usual = lambda k, d=d: act(*copies(d, k, from_hbm.at[d, part(k)]))
            aside = lambda k, d=d: act(*copies(d, k, late_hbm.at[part(k - main)]))
            loop(0, main, usual)
            away = n - 1 - me if d == n - 1 else me if d == 0 else None
            if away is None:
                loop(main, count, usual)
            else:
                pl.when(away < n - 2)(lambda usual=usual: loop(main, count, usual))
                pl.when(away == n - 2)(lambda aside=aside: loop(main, count, aside))

    def relay(take, put):
        take.wait()
        put.start()

    whole(lambda take, put: take.start())
    whole(relay)
    whole(lambda take, put: put.wait())


def place(gathered, late, row_new, col_new, late_chunks, chunk):
    n, flat, columns = gathered.shape
    hbm, vmem = pl.BlockSpec(memory_space=pltpu.HBM), pl.BlockSpec(memory_space=pltpu.VMEM)
    slots = n * (flat // chunk)
    return pl.pallas_call(
        functools.partial(place_kernel, late_chunks, chunk),
        in_specs=[hbm, hbm, vmem, vmem],
        out_specs=(hbm, vmem, vmem),
        out_shape=(
            jax.ShapeDtypeStruct((flat, n * columns), bf16),
            jax.ShapeDtypeStruct(row_new.shape, f32),
            jax.ShapeDtypeStruct(col_new.shape, f32),
        ),
        scratch_shapes=[
            pltpu.VMEM((n, flat, columns), bf16),
            pltpu.SemaphoreType.DMA((slots,)),
            pltpu.SemaphoreType.DMA((slots,)),
        ],
        compiler_params=pltpu.CompilerParams(vmem_limit_bytes=56 * 1024 * 1024),
        cost_estimate=pl.CostEstimate(
            flops=n * flat * columns, bytes_accessed=4 * n * flat * columns, transcendentals=0
        ),
    )(gathered, late, row_new, col_new)


def place_late_kernel(n, held_hbm, moved, out_hbm, sem):
    rows, columns = moved.shape
    there = pl.ds(out_hbm.shape[0] - rows, rows)
    for at, d in ((0, n - 1), (n - 1, 0)):

        @pl.when(lax.axis_index("gz") == at)
        def _(d=d):
            target = out_hbm.at[there, pl.ds(d * columns, columns)]
            copy = pltpu.make_async_copy(moved, target, sem)
            copy.start()
            copy.wait()


def place_late(held, moved, n):
    anywhere = pl.BlockSpec(memory_space=pl.ANY)
    rows, columns = moved.shape
    return pl.pallas_call(
        functools.partial(place_late_kernel, n),
        in_specs=[anywhere, pl.BlockSpec(memory_space=pltpu.VMEM)],
        out_specs=anywhere,
        out_shape=jax.ShapeDtypeStruct(held.shape, bf16),
        scratch_shapes=[pltpu.SemaphoreType.DMA],
        input_output_aliases={0: 0},
        compiler_params=pltpu.CompilerParams(vmem_limit_bytes=8 * 1024 * 1024),
        cost_estimate=pl.CostEstimate(
            flops=rows * columns, bytes_accessed=4 * rows * columns, transcendentals=0
        ),
    )(held, moved)


def body(params, grads, row_state, col_state):
    layers, rows, columns = params.shape
    n = lax.axis_size("gz")
    per, count, late_chunks, _ = cuts(layers, rows)
    row_new, col_new, row_root, col_step, gathered, late = step(
        params, grads, row_state, col_state
    )
    moved = lax.ppermute(late, "gz", [(n - 2, n - 1), (1, 0)])
    applied = grads.astype(f32) * row_root[:, :, None] * col_step[:, None, :]
    new_params = params - step_share * applied
    held, row_new, col_new = place(gathered, late, row_new, col_new, late_chunks, per * LANES)
    held = place_late(held, moved, n)
    compute = held.reshape(layers, rows, n * columns)
    return (new_params, row_new, col_new, applied, compute)


def solution(mesh):
    in_specs = (P("gx", "gy", "gz"), P("gx", "gy", "gz"), P("gx", "gy"), P("gx", "gz"))
    out_specs = (
        P("gx", "gy", "gz"),
        P("gx", "gy"),
        P("gx", "gz"),
        P("gx", "gy", "gz"),
        P("gx", "gy", None),
    )
    return jax.shard_map(body, mesh=mesh, in_specs=in_specs, out_specs=out_specs, check_vma=False)
```

```python
import functools
import itertools
import jax
import jax.numpy as jnp
from jax import lax
from jax.experimental import pallas as pl
from jax.experimental.pallas import tpu as pltpu
from jax.sharding import PartitionSpec as P

decay_rate = 0.842
tiny_term = 1e-30
step_share = 0.01
clip_limit = 1.0
LANES = 128
f32, bf16 = jnp.float32, jnp.bfloat16


def fold(values):
    return jnp.sum(values.reshape(values.shape[0] // 8, 8, values.shape[1]), axis=0)


def fold_lanes(row):
    return sum(row[:, i : i + LANES] for i in range(0, row.shape[1], LANES))


def down(row):
    return jnp.broadcast_to(row, (LANES, LANES)).T


def peers(axes):
    mine = [lax.axis_index(a) for a in axes]
    sizes = [lax.axis_size(a) for a in axes]
    for shift in itertools.product(*[range(n) for n in sizes]):
        if any(shift):
            yield {a: lax.rem(m + d, n) for a, m, d, n in zip(axes, mine, shift, sizes)}


def exchange(axes, mine, send, recv, base, act):
    for slot, device in enumerate(peers(axes)):
        act(
            pltpu.make_async_remote_copy(
                src_ref=mine,
                dst_ref=mine,
                send_sem=send.at[base + slot],
                recv_sem=recv.at[base + slot],
                device_id=device,
                device_id_type=pl.DeviceIdType.MESH,
            )
        )


def start(copy):
    copy.start()


def finish(copy):
    copy.wait()


def total(parts):
    return functools.reduce(lambda a, b: a + b, parts)


def loop(low, high, step):
    def one(k, carry):
        step(k)
        return carry

    lax.fori_loop(low, high, one, 0)


def step_kernel(
    layers, per, late, early,
    p_hbm, g_hbm, row_hbm, col_hbm,
    row_out, col_out, root_out, step_out, all_hbm, late_hbm,
    p_vm, g_vm, new_vm, row_vm, root_vm, old_col, col_vm, step_vm,
    row_all, col_all, sum_all, up_all, param_all, new_row, inverse, root,
    near_p, near_g, near_col, near_new,
    p_sem, g_sem, o_sem, small_in, small_out, near_s, near_r, near_o,
    rz_s, rz_r, cy_s, cy_r, sum_s, sum_r, up_s, up_r, param_s, param_r,
    right_s, right_r, left_s, left_r,
):
    flat, columns = g_vm.shape
    rows = flat // layers
    nb, chunk = rows // LANES, per * LANES
    chunks = nb // per
    count = layers * chunks
    nx, ny, nz = (lax.axis_size(a) for a in ("gx", "gy", "gz"))
    me_x, me_y, me_z = (lax.axis_index(a) for a in ("gx", "gy", "gz"))
    rows_all, columns_all = rows * ny, columns * nz

    def part(k):
        return pl.ds(pl.multiple_of(k * chunk, chunk), chunk)

    def block(b):
        return pl.ds(pl.multiple_of(b * LANES, LANES), LANES)

    def g_load(k):
        return pltpu.make_async_copy(g_hbm.at[part(k)], g_vm.at[part(k)], g_sem.at[k])

    def p_load(k):
        return pltpu.make_async_copy(p_hbm.at[part(k)], p_vm.at[part(k)], p_sem.at[k])

    sides = ((1, me_z, right_s, right_r), (-1, nz - 1 - me_z, left_s, left_r))

    loop(0, count, lambda k: g_load(k).start())
    olds = [
        pltpu.make_async_copy(row_hbm, row_vm, small_in.at[0]),
        pltpu.make_async_copy(col_hbm, old_col, small_in.at[1]),
    ]
    for copy in olds:
        copy.start()
    loop(0, count, lambda k: p_load(k).start())

    plane = ("gy", "gz")
    barrier = pltpu.get_barrier_semaphore()
    for device in itertools.chain(peers(plane), peers(("gx",))):
        pl.semaphore_signal(
            barrier, inc=1, device_id=device, device_id_type=pl.DeviceIdType.MESH
        )

    if per < 8:

        def clear(k):
            row_all[me_z, k, per:, :] = jnp.zeros((8 - per, LANES), f32)

        loop(0, count, clear)

    def rows_of(k, act):
        exchange(("gz",), row_all.at[me_z, k], rz_s, rz_r, k * (nz - 1), act)

    def columns_of(l, act):
        exchange(("gy",), col_all.at[me_y, l], cy_s, cy_r, l * (ny - 1), act)

    for l in range(layers):

        def measure_chunk(c, col_sum, l=l):
            k = l * chunks + c
            g_load(k).wait()
            for b in range(per):
                grad = g_vm[block(k * per + b), :].astype(f32)
                squares = grad * grad
                row_all[me_z, k, b : b + 1, :] = jnp.sum(
                    fold_lanes(squares).T, axis=0, keepdims=True
                )
                col_sum = col_sum + fold(squares)
            if l > 0:
                rows_of(k, start)
            return col_sum

        col_all[me_y, l] = lax.fori_loop(0, chunks, measure_chunk, jnp.zeros((8, columns), f32))
        if l == 0:
            pl.semaphore_wait(barrier, ny * nz + nx - 2)
            loop(0, chunks, lambda c: rows_of(c, start))
        columns_of(l, start)

    last = pl.ds(flat - early, early)
    first_rows = early // 48 * 16

    def near(side, act, which=(0, 1, 2, 3, 4)):
        head = pl.ds(flat - early, first_rows)
        rest = pl.ds(flat - early + first_rows, early - first_rows)
        head_to, rest_to = pl.ds(0, first_rows), pl.ds(first_rows, early - first_rows)
        moves = (
            (col_vm, near_col),
            (p_hbm.at[head], near_p.at[head_to]),
            (g_hbm.at[head], near_g.at[head_to]),
            (p_hbm.at[rest], near_p.at[rest_to]),
            (g_hbm.at[rest], near_g.at[rest_to]),
        )
        for i in which:
            source, target = moves[i]
            act(
                pltpu.make_async_remote_copy(
                    src_ref=source,
                    dst_ref=target,
                    send_sem=near_s.at[i],
                    recv_sem=near_r.at[i],
                    device_id={"gz": me_z + side[0]},
                    device_id_type=pl.DeviceIdType.MESH,
                )
            )

    for side in sides:
        pl.when(side[1] == nz - 2)(lambda side=side: near(side, start, (1, 2)))

    for copy in olds:
        copy.wait()
    for l in range(layers):
        for b in range(nb):
            new_row[l * chunks + b // per, b % per : b % per + 1, :] = row_vm[
                l : l + 1, b * LANES : (b + 1) * LANES
            ]

    packed = jnp.zeros((2, LANES), f32)
    lane = lax.broadcasted_iota(jnp.int32, (2, LANES), 1)
    line = lax.broadcasted_iota(jnp.int32, (2, LANES), 0)

    def pack(packed, at_line, at_lane, values):
        value = jnp.sum(jnp.sum(values, axis=0, keepdims=True), axis=1, keepdims=True)
        return jnp.where(jnp.logical_and(line == at_line, lane == at_lane), value, packed)

    for l in range(layers):

        columns_of(l, finish)
        col_sum = jnp.sum(total([col_all[y, l] for y in range(ny)]), axis=0, keepdims=True)
        col_now = decay_rate * old_col[l : l + 1, :] + (1.0 - decay_rate) * (
            col_sum / rows_all + tiny_term
        )
        col_vm[l : l + 1, :] = col_now
        inverse_col = 1.0 / col_now

        def weigh_chunk(c, carry, l=l, inverse_col=inverse_col):
            acc, row_sum = carry
            k = l * chunks + c
            rows_of(k, finish)
            squares = total([row_all[z, k, 0:per, :] for z in range(nz)]) / columns_all + tiny_term
            row_now = decay_rate * new_row[k, 0:per, :] + (1.0 - decay_rate) * squares
            new_row[k, 0:per, :] = row_now
            inverse[k, 0:per, :] = 1.0 / row_now
            root[k, 0:per, :] = lax.rsqrt(row_now)
            for b in range(per):
                grad = g_vm[block(k * per + b), :].astype(f32)
                share = fold_lanes(grad * grad * inverse_col)
                acc = acc + fold(share * down(inverse[k, b : b + 1, :]))
            return acc, row_sum + row_now

        acc, row_sum = lax.fori_loop(
            0, chunks, weigh_chunk, (jnp.zeros((8, LANES), f32), jnp.zeros((per, LANES), f32))
        )
        packed = pack(packed, 0, l, acc)
        packed = pack(packed, 1, l, row_sum)

    sum_all[me_y, me_z] = packed
    exchange(plane, sum_all.at[me_y, me_z], sum_s, sum_r, 0, start)

    col_root = lax.rsqrt(col_vm[...])

    packed = jnp.zeros((2, LANES), f32)
    for l in range(layers):

        def params_chunk(c, acc, l=l):
            k = l * chunks + c
            p_load(k).wait()
            for b in range(per):
                weights = p_vm[block(k * per + b), :]
                acc = acc + fold(fold_lanes(weights * weights))
            return acc

        params_sum = lax.fori_loop(0, chunks, params_chunk, jnp.zeros((8, LANES), f32))
        packed = pack(packed, 0, l, params_sum)
    param_all[me_y, me_z] = packed
    exchange(plane, param_all.at[me_y, me_z], param_s, param_r, 0, start)
    for side in sides:
        pl.when(side[1] == nz - 2)(lambda side=side: near(side, start, (0, 3, 4)))

    exchange(plane, sum_all.at[me_y, me_z], sum_s, sum_r, 0, finish)
    here = total([sum_all[y, z] for y in range(ny) for z in range(nz)])
    both = jnp.where(lane[0:1] < layers, here[0:1] * here[1:2], 0.0)
    up_all[me_x] = jnp.broadcast_to(both, (2, LANES))
    exchange(("gx",), up_all.at[me_x], up_s, up_r, 0, start)
    exchange(plane, param_all.at[me_y, me_z], param_s, param_r, 0, finish)
    params_sums = total([param_all[y, z, 0:1] for y in range(ny) for z in range(nz)])
    parts, scales = [], []
    for l in range(layers):
        row_mean = here[1:2, l : l + 1] / (nz * rows_all)
        weight_scale = jnp.sqrt(params_sums[:, l : l + 1] / (rows_all * columns_all))
        scales.append(jnp.sqrt(row_mean) * weight_scale)
        parts.append(col_root[l : l + 1] * scales[l])
    exchange(("gx",), up_all.at[me_x], up_s, up_r, 0, finish)
    update_sum = total([up_all[x, 0:1] for x in range(nx)])
    update_total = jnp.sum(update_sum, axis=1, keepdims=True) / (nz * rows_all)
    entries = layers * nx * rows_all * columns_all
    clip_factor = jnp.maximum(1.0, jnp.sqrt(update_total / entries) / clip_limit)
    for l in range(layers):
        step_vm[l : l + 1, :] = parts[l] / clip_factor
    less = step_vm[...] * step_share

    def late_part(k):
        return pl.ds(pl.multiple_of((k - (count - late)) * chunk, chunk), chunk)

    def size_of(k, short):
        return pl.ds(pl.multiple_of(k * chunk, chunk), chunk - early) if short else part(k)

    def hop(side, s, k, to_late=False, short=False):
        way, _, send, recv = side
        shard = me_z - way * (s - 1)
        slot = (s - 1) * count + k
        rows_k = size_of(k, short)
        target = late_hbm.at[late_part(k)] if to_late else all_hbm.at[shard, rows_k]
        return pltpu.make_async_remote_copy(
            src_ref=new_vm.at[rows_k] if s == 1 else all_hbm.at[shard, rows_k],
            dst_ref=target,
            send_sem=send.at[slot],
            recv_sem=recv.at[slot],
            device_id={"gz": me_z + way},
            device_id_type=pl.DeviceIdType.MESH,
        )

    def arrival(side, s, k, short=False):
        way, _, send, recv = side
        slot = (s - 1) * count + k
        here = all_hbm.at[me_z - way * s, size_of(k, short)]
        return pltpu.make_async_remote_copy(
            src_ref=here,
            dst_ref=here,
            send_sem=send.at[slot],
            recv_sem=recv.at[slot],
            device_id={"gz": me_z + way},
            device_id_type=pl.DeviceIdType.MESH,
        )

    def for_arrival(side, s, k, final):
        if final:
            pl.when(side[1] == nz - 1)(lambda: arrival(side, s, k, True).wait_recv())
            full = jnp.logical_and(side[1] >= s, side[1] < nz - 1)
        else:
            full = side[1] >= s
        pl.when(full)(lambda: arrival(side, s, k).wait_recv())

    def for_hop(side, s, k, is_late, act, final=False):
        place = side[1]
        if s == nz - 1 and is_late:
            return
        if s == nz - 2 and is_late:

            @pl.when(place == nz - 3)
            def _():
                act(hop(side, s, k, True))

            @pl.when(place == nz - 2)
            def _():
                act(hop(side, s, k))

        elif final:

            @pl.when(place < nz - 2)
            def _():
                act(hop(side, s, k))

            @pl.when(place == nz - 2)
            def _():
                act(hop(side, s, k, short=True))

        else:

            @pl.when(jnp.logical_and(place >= s - 1, place < nz - 1))
            def _():
                act(hop(side, s, k))

    def own(k):
        return pltpu.make_async_copy(new_vm.at[part(k)], all_hbm.at[me_z, part(k)], o_sem.at[k])

    def launch(k, final=False):
        for side in sides:
            for_hop(side, 1, k, False, start, final)
        own(k).start()

    for l in range(layers):

        def apply_chunk(c, l=l):
            k = l * chunks + c

            for b in range(per):
                here = block(k * per + b)
                factor = down(root[k, b : b + 1, :])
                for j in range(0, columns, LANES):
                    cut = slice(j, j + LANES)
                    taken = g_vm[here, cut].astype(f32) * factor * less[l : l + 1, cut]
                    new_vm[here, cut] = (p_vm[here, cut] - taken).astype(bf16)
                if b == min(1, per - 1):
                    pl.when(k > 0)(lambda: launch(k - 1))

        loop(0, chunks, apply_chunk)
    launch(count - 1, True)

    def near_rows(side):
        near(side, lambda copy: copy.wait_recv())
        l, k = layers - 1, count - 1
        near_less = lax.rsqrt(near_col[l : l + 1, :]) * scales[l] / clip_factor * step_share
        skip = chunk - early
        for b in range(skip // LANES, per):
            low = max(0, skip - b * LANES)
            rows_b = slice(b * LANES + low - skip, (b + 1) * LANES - skip)
            factor = down(root[k, b : b + 1, :])[low:, :]
            for j in range(0, columns, LANES):
                cut = slice(j, j + LANES)
                taken = near_g[rows_b, cut].astype(f32) * factor * near_less[:, cut]
                near_new[rows_b, cut] = (near_p[rows_b, cut] - taken).astype(bf16)

    def near_put(side):
        return pltpu.make_async_copy(near_new, all_hbm.at[me_z - side[0], last], near_o)

    for side in sides:
        pl.when(side[1] == nz - 1)(lambda side=side: near_rows(side))
        pl.when(side[1] == nz - 2)(lambda side=side: near(side, lambda copy: copy.wait_send()))

    for l in range(layers):
        for b in range(nb):
            cut = slice(b * LANES, (b + 1) * LANES)
            k, i = l * chunks + b // per, b % per
            row_vm[l : l + 1, cut] = new_row[k, i : i + 1, :]
            root_vm[l : l + 1, cut] = root[k, i : i + 1, :]
    smalls = [
        pltpu.make_async_copy(source, target, small_out.at[i])
        for i, (source, target) in enumerate(
            ((row_vm, row_out), (col_vm, col_out), (root_vm, root_out), (step_vm, step_out))
        )
    ]
    for copy in smalls:
        copy.start()

    for side in sides:
        pl.when(side[1] == nz - 1)(lambda side=side: near_put(side).start())

    def pass_on(s, k, is_late, final=False):
        for side in sides:
            for_arrival(side, s, k, final)
            if s + 1 < nz:
                for_hop(side, s + 1, k, is_late, start)
        for side in sides:
            for_hop(side, s, k, is_late, lambda copy: copy.wait_send(), final)

    for s in range(1, nz):
        if s == nz - 1:
            loop(0, count, lambda k: own(k).wait())
            for copy in smalls:
                copy.wait()
            for side in sides:
                pl.when(side[1] == nz - 1)(lambda side=side: near_put(side).wait())
        loop(0, count - late, lambda k, s=s: pass_on(s, k, False))
        if s == 1:
            loop(count - late, count - 1, lambda k: pass_on(1, k, True))
            pass_on(1, count - 1, True, True)
        elif s < nz - 1:
            loop(count - late, count, lambda k, s=s: pass_on(s, k, True))


def cuts(layers, rows):
    nb = rows // LANES
    per = max(q for q in range(1, 9) if nb % q == 0)
    count = layers * (nb // per)
    return per, count, max(1, count // 3), min(192, (per - 1) * LANES)


def step(params, grads, row_state, col_state):
    layers, rows, columns = params.shape
    nx, ny, nz = (lax.axis_size(a) for a in ("gx", "gy", "gz"))
    assert nz > 3
    flat = layers * rows
    per, count, late, early = cuts(layers, rows)
    sem = lambda n: pltpu.SemaphoreType.DMA((max(n, 1),))
    anywhere = pl.BlockSpec(memory_space=pl.ANY)
    pairs = [count * (nz - 1), layers * (ny - 1), ny * nz - 1, nx - 1, ny * nz - 1] + [(nz - 1) * count] * 2
    return pl.pallas_call(
        functools.partial(step_kernel, layers, per, late, early),
        out_shape=(
            jax.ShapeDtypeStruct((layers, rows), f32),
            jax.ShapeDtypeStruct((layers, columns), f32),
            jax.ShapeDtypeStruct((layers, rows), f32),
            jax.ShapeDtypeStruct((layers, columns), f32),
            jax.ShapeDtypeStruct((nz, flat, columns), bf16),
            jax.ShapeDtypeStruct((late * per * LANES, columns), bf16),
        ),
        in_specs=[anywhere] * 4,
        out_specs=(anywhere,) * 6,
        scratch_shapes=[
            pltpu.VMEM((flat, columns), f32),
            pltpu.VMEM((flat, columns), bf16),
            pltpu.VMEM((flat, columns), bf16),
            pltpu.VMEM((layers, rows), f32),
            pltpu.VMEM((layers, rows), f32),
            pltpu.VMEM((layers, columns), f32),
            pltpu.VMEM((layers, columns), f32),
            pltpu.VMEM((layers, columns), f32),
            pltpu.VMEM((nz, count, 8, LANES), f32),
            pltpu.VMEM((ny, layers, 8, columns), f32),
            pltpu.VMEM((ny, nz, 2, LANES), f32),
            pltpu.VMEM((nx, 2, LANES), f32),
            pltpu.VMEM((ny, nz, 2, LANES), f32),
            pltpu.VMEM((count, 8, LANES), f32),
            pltpu.VMEM((count, 8, LANES), f32),
            pltpu.VMEM((count, 8, LANES), f32),
            pltpu.VMEM((early, columns), f32),
            pltpu.VMEM((early, columns), bf16),
            pltpu.VMEM((layers, columns), f32),
            pltpu.VMEM((early, columns), bf16),
            sem(count),
            sem(count),
            sem(count),
            sem(2),
            sem(4),
            sem(5),
            sem(5),
            pltpu.SemaphoreType.DMA,
        ]
        + [sem(n) for n in pairs for _ in range(2)],
        compiler_params=pltpu.CompilerParams(
            collective_id=0, has_side_effects=True, vmem_limit_bytes=60 * 1024 * 1024
        ),
        cost_estimate=pl.CostEstimate(
            flops=20 * flat * columns, bytes_accessed=8 * flat * columns, transcendentals=0
        ),
    )(params.reshape(flat, columns), grads.reshape(flat, columns), row_state, col_state)


def place_kernel(
    late_chunks, chunk, from_hbm, late_hbm, row_in, col_in,
    out_hbm, row_out, col_out, stage, in_sem, out_sem,
):
    n, flat, columns = from_hbm.shape
    count, me = flat // chunk, lax.axis_index("gz")
    main = count - late_chunks
    row_out[...] = row_in[...]
    col_out[...] = col_in[...]

    def part(k):
        return pl.ds(pl.multiple_of(k * chunk, chunk), chunk)

    def copies(d, k, source):
        slot = d * count + k
        return (
            pltpu.make_async_copy(source, stage.at[d, part(k)], in_sem.at[slot]),
            pltpu.make_async_copy(
                stage.at[d, part(k)],
                out_hbm.at[part(k), pl.ds(d * columns, columns)],
                out_sem.at[slot],
            ),
        )

    def whole(act):
        for d in range(n):
            usual = lambda k, d=d: act(*copies(d, k, from_hbm.at[d, part(k)]))
            aside = lambda k, d=d: act(*copies(d, k, late_hbm.at[part(k - main)]))
            loop(0, main, usual)
            away = n - 1 - me if d == n - 1 else me if d == 0 else None
            if away is None:
                loop(main, count, usual)
            else:
                pl.when(away < n - 2)(lambda usual=usual: loop(main, count, usual))
                pl.when(away == n - 2)(lambda aside=aside: loop(main, count, aside))

    def relay(take, put):
        take.wait()
        put.start()

    whole(lambda take, put: take.start())
    whole(relay)
    whole(lambda take, put: put.wait())


def place(gathered, late, row_new, col_new, late_chunks, chunk):
    n, flat, columns = gathered.shape
    hbm, vmem = pl.BlockSpec(memory_space=pltpu.HBM), pl.BlockSpec(memory_space=pltpu.VMEM)
    slots = n * (flat // chunk)
    return pl.pallas_call(
        functools.partial(place_kernel, late_chunks, chunk),
        in_specs=[hbm, hbm, vmem, vmem],
        out_specs=(hbm, vmem, vmem),
        out_shape=(
            jax.ShapeDtypeStruct((flat, n * columns), bf16),
            jax.ShapeDtypeStruct(row_new.shape, f32),
            jax.ShapeDtypeStruct(col_new.shape, f32),
        ),
        scratch_shapes=[
            pltpu.VMEM((n, flat, columns), bf16),
            pltpu.SemaphoreType.DMA((slots,)),
            pltpu.SemaphoreType.DMA((slots,)),
        ],
        compiler_params=pltpu.CompilerParams(vmem_limit_bytes=56 * 1024 * 1024),
        cost_estimate=pl.CostEstimate(
            flops=n * flat * columns, bytes_accessed=4 * n * flat * columns, transcendentals=0
        ),
    )(gathered, late, row_new, col_new)


def place_late_kernel(n, held_hbm, moved, out_hbm, sem):
    rows, columns = moved.shape
    there = pl.ds(out_hbm.shape[0] - rows, rows)
    for at, d in ((0, n - 1), (n - 1, 0)):

        @pl.when(lax.axis_index("gz") == at)
        def _(d=d):
            target = out_hbm.at[there, pl.ds(d * columns, columns)]
            copy = pltpu.make_async_copy(moved, target, sem)
            copy.start()
            copy.wait()


def place_late(held, moved, n):
    anywhere = pl.BlockSpec(memory_space=pl.ANY)
    rows, columns = moved.shape
    return pl.pallas_call(
        functools.partial(place_late_kernel, n),
        in_specs=[anywhere, pl.BlockSpec(memory_space=pltpu.VMEM)],
        out_specs=anywhere,
        out_shape=jax.ShapeDtypeStruct(held.shape, bf16),
        scratch_shapes=[pltpu.SemaphoreType.DMA],
        input_output_aliases={0: 0},
        compiler_params=pltpu.CompilerParams(vmem_limit_bytes=8 * 1024 * 1024),
        cost_estimate=pl.CostEstimate(
            flops=rows * columns, bytes_accessed=4 * rows * columns, transcendentals=0
        ),
    )(held, moved)


def body(params, grads, row_state, col_state):
    layers, rows, columns = params.shape
    n = lax.axis_size("gz")
    per, count, late_chunks, _ = cuts(layers, rows)
    row_new, col_new, row_root, col_step, gathered, late = step(
        params, grads, row_state, col_state
    )
    moved = lax.ppermute(late, "gz", [(n - 2, n - 1), (1, 0)])
    applied = grads.astype(f32) * row_root[:, :, None] * col_step[:, None, :]
    new_params = params - step_share * applied
    held, row_new, col_new = place(gathered, late, row_new, col_new, late_chunks, per * LANES)
    held = place_late(held, moved, n)
    compute = held.reshape(layers, rows, n * columns)
    return (new_params, row_new, col_new, applied, compute)


def solution(mesh):
    in_specs = (P("gx", "gy", "gz"), P("gx", "gy", "gz"), P("gx", "gy"), P("gx", "gz"))
    out_specs = (
        P("gx", "gy", "gz"),
        P("gx", "gy"),
        P("gx", "gz"),
        P("gx", "gy", "gz"),
        P("gx", "gy", None),
    )
    return jax.shard_map(body, mesh=mesh, in_specs=in_specs, out_specs=out_specs, check_vma=False)
```

```python
import functools
import itertools
import jax
import jax.numpy as jnp
from jax import lax
from jax.experimental import pallas as pl
from jax.experimental.pallas import tpu as pltpu
from jax.sharding import PartitionSpec as P

decay_rate = 0.842
tiny_term = 1e-30
step_share = 0.01
clip_limit = 1.0
LANES = 128
f32, bf16 = jnp.float32, jnp.bfloat16


def fold(values):
    return jnp.sum(values.reshape(values.shape[0] // 8, 8, values.shape[1]), axis=0)


def fold_lanes(row):
    return sum(row[:, i : i + LANES] for i in range(0, row.shape[1], LANES))


def down(row):
    return jnp.broadcast_to(row, (LANES, LANES)).T


def peers(axes):
    mine = [lax.axis_index(a) for a in axes]
    sizes = [lax.axis_size(a) for a in axes]
    for shift in itertools.product(*[range(n) for n in sizes]):
        if any(shift):
            yield {a: lax.rem(m + d, n) for a, m, d, n in zip(axes, mine, shift, sizes)}


def exchange(axes, mine, send, recv, base, act):
    for slot, device in enumerate(peers(axes)):
        act(
            pltpu.make_async_remote_copy(
                src_ref=mine,
                dst_ref=mine,
                send_sem=send.at[base + slot],
                recv_sem=recv.at[base + slot],
                device_id=device,
                device_id_type=pl.DeviceIdType.MESH,
            )
        )


def start(copy):
    copy.start()


def finish(copy):
    copy.wait()


def total(parts):
    return functools.reduce(lambda a, b: a + b, parts)


def loop(low, high, step):
    def one(k, carry):
        step(k)
        return carry

    lax.fori_loop(low, high, one, 0)


def step_kernel(
    layers, per, late, early,
    p_hbm, g_hbm, row_hbm, col_hbm,
    row_out, col_out, root_out, step_out, all_hbm, late_hbm,
    p_vm, g_vm, new_vm, row_vm, root_vm, old_col, col_vm, step_vm,
    row_all, col_all, sum_all, up_all, param_all, new_row, inverse, root,
    near_p, near_g, near_col, near_new,
    p_sem, g_sem, o_sem, small_in, small_out, near_s, near_r, near_o,
    rz_s, rz_r, cy_s, cy_r, sum_s, sum_r, up_s, up_r, param_s, param_r,
    right_s, right_r, left_s, left_r,
):
    flat, columns = g_vm.shape
    rows = flat // layers
    nb, chunk = rows // LANES, per * LANES
    chunks = nb // per
    count = layers * chunks
    nx, ny, nz = (lax.axis_size(a) for a in ("gx", "gy", "gz"))
    me_x, me_y, me_z = (lax.axis_index(a) for a in ("gx", "gy", "gz"))
    rows_all, columns_all = rows * ny, columns * nz

    def part(k):
        return pl.ds(pl.multiple_of(k * chunk, chunk), chunk)

    def block(b):
        return pl.ds(pl.multiple_of(b * LANES, LANES), LANES)

    def g_load(k):
        return pltpu.make_async_copy(g_hbm.at[part(k)], g_vm.at[part(k)], g_sem.at[k])

    def p_load(k):
        return pltpu.make_async_copy(p_hbm.at[part(k)], p_vm.at[part(k)], p_sem.at[k])

    sides = ((1, me_z, right_s, right_r), (-1, nz - 1 - me_z, left_s, left_r))

    loop(0, count, lambda k: g_load(k).start())
    olds = [
        pltpu.make_async_copy(row_hbm, row_vm, small_in.at[0]),
        pltpu.make_async_copy(col_hbm, old_col, small_in.at[1]),
    ]
    for copy in olds:
        copy.start()
    loop(0, count, lambda k: p_load(k).start())

    plane = ("gy", "gz")
    barrier = pltpu.get_barrier_semaphore()
    for device in itertools.chain(peers(plane), peers(("gx",))):
        pl.semaphore_signal(
            barrier, inc=1, device_id=device, device_id_type=pl.DeviceIdType.MESH
        )

    if per < 8:

        def clear(k):
            row_all[me_z, k, per:, :] = jnp.zeros((8 - per, LANES), f32)

        loop(0, count, clear)

    def rows_of(k, act):
        exchange(("gz",), row_all.at[me_z, k], rz_s, rz_r, k * (nz - 1), act)

    def columns_of(l, act):
        exchange(("gy",), col_all.at[me_y, l], cy_s, cy_r, l * (ny - 1), act)

    for l in range(layers):

        def measure_chunk(c, col_sum, l=l):
            k = l * chunks + c
            g_load(k).wait()
            for b in range(per):
                grad = g_vm[block(k * per + b), :].astype(f32)
                squares = grad * grad
                row_all[me_z, k, b : b + 1, :] = jnp.sum(
                    fold_lanes(squares).T, axis=0, keepdims=True
                )
                col_sum = col_sum + fold(squares)
            if l > 0:
                rows_of(k, start)
            return col_sum

        col_all[me_y, l] = lax.fori_loop(0, chunks, measure_chunk, jnp.zeros((8, columns), f32))
        if l == 0:
            pl.semaphore_wait(barrier, ny * nz + nx - 2)
            loop(0, chunks, lambda c: rows_of(c, start))
        columns_of(l, start)

    last = pl.ds(flat - early, early)
    first_rows = early // 48 * 16

    def near(side, act, which=(0, 1, 2, 3, 4)):
        head = pl.ds(flat - early, first_rows)
        rest = pl.ds(flat - early + first_rows, early - first_rows)
        head_to, rest_to = pl.ds(0, first_rows), pl.ds(first_rows, early - first_rows)
        moves = (
            (col_vm, near_col),
            (p_hbm.at[head], near_p.at[head_to]),
            (g_hbm.at[head], near_g.at[head_to]),
            (p_hbm.at[rest], near_p.at[rest_to]),
            (g_hbm.at[rest], near_g.at[rest_to]),
        )
        for i in which:
            source, target = moves[i]
            act(
                pltpu.make_async_remote_copy(
                    src_ref=source,
                    dst_ref=target,
                    send_sem=near_s.at[i],
                    recv_sem=near_r.at[i],
                    device_id={"gz": me_z + side[0]},
                    device_id_type=pl.DeviceIdType.MESH,
                )
            )

    for side in sides:
        pl.when(side[1] == nz - 2)(lambda side=side: near(side, start, (1, 2)))

    for copy in olds:
        copy.wait()
    for l in range(layers):
        for b in range(nb):
            new_row[l * chunks + b // per, b % per : b % per + 1, :] = row_vm[
                l : l + 1, b * LANES : (b + 1) * LANES
            ]

    packed = jnp.zeros((2, LANES), f32)
    lane = lax.broadcasted_iota(jnp.int32, (2, LANES), 1)
    line = lax.broadcasted_iota(jnp.int32, (2, LANES), 0)

    def pack(packed, at_line, at_lane, values):
        value = jnp.sum(jnp.sum(values, axis=0, keepdims=True), axis=1, keepdims=True)
        return jnp.where(jnp.logical_and(line == at_line, lane == at_lane), value, packed)

    for l in range(layers):

        columns_of(l, finish)
        col_sum = jnp.sum(total([col_all[y, l] for y in range(ny)]), axis=0, keepdims=True)
        col_now = decay_rate * old_col[l : l + 1, :] + (1.0 - decay_rate) * (
            col_sum / rows_all + tiny_term
        )
        col_vm[l : l + 1, :] = col_now
        inverse_col = 1.0 / col_now

        def weigh_chunk(c, carry, l=l, inverse_col=inverse_col):
            acc, row_sum = carry
            k = l * chunks + c
            rows_of(k, finish)
            squares = total([row_all[z, k, 0:per, :] for z in range(nz)]) / columns_all + tiny_term
            row_now = decay_rate * new_row[k, 0:per, :] + (1.0 - decay_rate) * squares
            new_row[k, 0:per, :] = row_now
            inverse[k, 0:per, :] = 1.0 / row_now
            root[k, 0:per, :] = lax.rsqrt(row_now)
            for b in range(per):
                grad = g_vm[block(k * per + b), :].astype(f32)
                share = fold_lanes(grad * grad * inverse_col)
                acc = acc + fold(share * down(inverse[k, b : b + 1, :]))
            return acc, row_sum + row_now

        acc, row_sum = lax.fori_loop(
            0, chunks, weigh_chunk, (jnp.zeros((8, LANES), f32), jnp.zeros((per, LANES), f32))
        )
        packed = pack(packed, 0, l, acc)
        packed = pack(packed, 1, l, row_sum)

    sum_all[me_y, me_z] = packed
    exchange(plane, sum_all.at[me_y, me_z], sum_s, sum_r, 0, start)

    col_root = lax.rsqrt(col_vm[...])

    packed = jnp.zeros((2, LANES), f32)
    for l in range(layers):

        def params_chunk(c, acc, l=l):
            k = l * chunks + c
            p_load(k).wait()
            for b in range(per):
                weights = p_vm[block(k * per + b), :]
                acc = acc + fold(fold_lanes(weights * weights))
            return acc

        params_sum = lax.fori_loop(0, chunks, params_chunk, jnp.zeros((8, LANES), f32))
        packed = pack(packed, 0, l, params_sum)
    param_all[me_y, me_z] = packed
    exchange(plane, param_all.at[me_y, me_z], param_s, param_r, 0, start)
    for side in sides:
        pl.when(side[1] == nz - 2)(lambda side=side: near(side, start, (0, 3, 4)))

    exchange(plane, sum_all.at[me_y, me_z], sum_s, sum_r, 0, finish)
    here = total([sum_all[y, z] for y in range(ny) for z in range(nz)])
    both = jnp.where(lane[0:1] < layers, here[0:1] * here[1:2], 0.0)
    up_all[me_x] = jnp.broadcast_to(both, (2, LANES))
    exchange(("gx",), up_all.at[me_x], up_s, up_r, 0, start)
    exchange(plane, param_all.at[me_y, me_z], param_s, param_r, 0, finish)
    params_sums = total([param_all[y, z, 0:1] for y in range(ny) for z in range(nz)])
    parts, scales = [], []
    for l in range(layers):
        row_mean = here[1:2, l : l + 1] / (nz * rows_all)
        weight_scale = jnp.sqrt(params_sums[:, l : l + 1] / (rows_all * columns_all))
        scales.append(jnp.sqrt(row_mean) * weight_scale)
        parts.append(col_root[l : l + 1] * scales[l])
    exchange(("gx",), up_all.at[me_x], up_s, up_r, 0, finish)
    update_sum = total([up_all[x, 0:1] for x in range(nx)])
    update_total = jnp.sum(update_sum, axis=1, keepdims=True) / (nz * rows_all)
    entries = layers * nx * rows_all * columns_all
    clip_factor = jnp.maximum(1.0, jnp.sqrt(update_total / entries) / clip_limit)
    for l in range(layers):
        step_vm[l : l + 1, :] = parts[l] / clip_factor
    less = step_vm[...] * step_share

    def late_part(k):
        return pl.ds(pl.multiple_of((k - (count - late)) * chunk, chunk), chunk)

    def size_of(k, short):
        return pl.ds(pl.multiple_of(k * chunk, chunk), chunk - early) if short else part(k)

    def hop(side, s, k, to_late=False, short=False):
        way, _, send, recv = side
        shard = me_z - way * (s - 1)
        slot = (s - 1) * count + k
        rows_k = size_of(k, short)
        target = late_hbm.at[late_part(k)] if to_late else all_hbm.at[shard, rows_k]
        return pltpu.make_async_remote_copy(
            src_ref=new_vm.at[rows_k] if s == 1 else all_hbm.at[shard, rows_k],
            dst_ref=target,
            send_sem=send.at[slot],
            recv_sem=recv.at[slot],
            device_id={"gz": me_z + way},
            device_id_type=pl.DeviceIdType.MESH,
        )

    def arrival(side, s, k, short=False):
        way, _, send, recv = side
        slot = (s - 1) * count + k
        here = all_hbm.at[me_z - way * s, size_of(k, short)]
        return pltpu.make_async_remote_copy(
            src_ref=here,
            dst_ref=here,
            send_sem=send.at[slot],
            recv_sem=recv.at[slot],
            device_id={"gz": me_z + way},
            device_id_type=pl.DeviceIdType.MESH,
        )

    def for_arrival(side, s, k, final):
        if final:
            pl.when(side[1] == nz - 1)(lambda: arrival(side, s, k, True).wait_recv())
            full = jnp.logical_and(side[1] >= s, side[1] < nz - 1)
        else:
            full = side[1] >= s
        pl.when(full)(lambda: arrival(side, s, k).wait_recv())

    def for_hop(side, s, k, is_late, act, final=False):
        place = side[1]
        if s == nz - 1 and is_late:
            return
        if s == nz - 2 and is_late:

            @pl.when(place == nz - 3)
            def _():
                act(hop(side, s, k, True))

            @pl.when(place == nz - 2)
            def _():
                act(hop(side, s, k))

        elif final:

            @pl.when(place < nz - 2)
            def _():
                act(hop(side, s, k))

            @pl.when(place == nz - 2)
            def _():
                act(hop(side, s, k, short=True))

        else:

            @pl.when(jnp.logical_and(place >= s - 1, place < nz - 1))
            def _():
                act(hop(side, s, k))

    def own(k):
        return pltpu.make_async_copy(new_vm.at[part(k)], all_hbm.at[me_z, part(k)], o_sem.at[k])

    def launch(k, final=False):
        for side in sides:
            for_hop(side, 1, k, False, start, final)
        own(k).start()

    for l in range(layers):

        def apply_chunk(c, l=l):
            k = l * chunks + c

            for b in range(per):
                here = block(k * per + b)
                factor = down(root[k, b : b + 1, :])
                for j in range(0, columns, LANES):
                    cut = slice(j, j + LANES)
                    taken = g_vm[here, cut].astype(f32) * factor * less[l : l + 1, cut]
                    new_vm[here, cut] = (p_vm[here, cut] - taken).astype(bf16)
                if b == min(1, per - 1):
                    pl.when(k > 0)(lambda: launch(k - 1))

        loop(0, chunks, apply_chunk)
    launch(count - 1, True)

    def near_rows(side):
        near(side, lambda copy: copy.wait_recv())
        l, k = layers - 1, count - 1
        near_less = lax.rsqrt(near_col[l : l + 1, :]) * scales[l] / clip_factor * step_share
        skip = chunk - early
        for b in range(skip // LANES, per):
            low = max(0, skip - b * LANES)
            rows_b = slice(b * LANES + low - skip, (b + 1) * LANES - skip)
            factor = down(root[k, b : b + 1, :])[low:, :]
            for j in range(0, columns, LANES):
                cut = slice(j, j + LANES)
                taken = near_g[rows_b, cut].astype(f32) * factor * near_less[:, cut]
                near_new[rows_b, cut] = (near_p[rows_b, cut] - taken).astype(bf16)

    def near_put(side):
        return pltpu.make_async_copy(near_new, all_hbm.at[me_z - side[0], last], near_o)

    for side in sides:
        pl.when(side[1] == nz - 1)(lambda side=side: near_rows(side))
        pl.when(side[1] == nz - 2)(lambda side=side: near(side, lambda copy: copy.wait_send()))

    for l in range(layers):
        for b in range(nb):
            cut = slice(b * LANES, (b + 1) * LANES)
            k, i = l * chunks + b // per, b % per
            row_vm[l : l + 1, cut] = new_row[k, i : i + 1, :]
            root_vm[l : l + 1, cut] = root[k, i : i + 1, :]
    smalls = [
        pltpu.make_async_copy(source, target, small_out.at[i])
        for i, (source, target) in enumerate(
            ((row_vm, row_out), (col_vm, col_out), (root_vm, root_out), (step_vm, step_out))
        )
    ]
    for copy in smalls:
        copy.start()

    for side in sides:
        pl.when(side[1] == nz - 1)(lambda side=side: near_put(side).start())

    def pass_on(s, k, is_late, final=False):
        for side in sides:
            for_arrival(side, s, k, final)
            if s + 1 < nz:
                for_hop(side, s + 1, k, is_late, start)
        for side in sides:
            for_hop(side, s, k, is_late, lambda copy: copy.wait_send(), final)

    for s in range(1, nz):
        if s == nz - 1:
            loop(0, count, lambda k: own(k).wait())
            for copy in smalls:
                copy.wait()
            for side in sides:
                pl.when(side[1] == nz - 1)(lambda side=side: near_put(side).wait())
        loop(0, count - late, lambda k, s=s: pass_on(s, k, False))
        if s == 1:
            loop(count - late, count - 1, lambda k: pass_on(1, k, True))
            pass_on(1, count - 1, True, True)
        elif s < nz - 1:
            loop(count - late, count, lambda k, s=s: pass_on(s, k, True))


def cuts(layers, rows):
    nb = rows // LANES
    per = max(q for q in range(1, 9) if nb % q == 0)
    count = layers * (nb // per)
    return per, count, max(1, count // 4), min(192, (per - 1) * LANES)


def step(params, grads, row_state, col_state):
    layers, rows, columns = params.shape
    nx, ny, nz = (lax.axis_size(a) for a in ("gx", "gy", "gz"))
    assert nz > 3
    flat = layers * rows
    per, count, late, early = cuts(layers, rows)
    sem = lambda n: pltpu.SemaphoreType.DMA((max(n, 1),))
    anywhere = pl.BlockSpec(memory_space=pl.ANY)
    pairs = [count * (nz - 1), layers * (ny - 1), ny * nz - 1, nx - 1, ny * nz - 1] + [(nz - 1) * count] * 2
    return pl.pallas_call(
        functools.partial(step_kernel, layers, per, late, early),
        out_shape=(
            jax.ShapeDtypeStruct((layers, rows), f32),
            jax.ShapeDtypeStruct((layers, columns), f32),
            jax.ShapeDtypeStruct((layers, rows), f32),
            jax.ShapeDtypeStruct((layers, columns), f32),
            jax.ShapeDtypeStruct((nz, flat, columns), bf16),
            jax.ShapeDtypeStruct((late * per * LANES, columns), bf16),
        ),
        in_specs=[anywhere] * 4,
        out_specs=(anywhere,) * 6,
        scratch_shapes=[
            pltpu.VMEM((flat, columns), f32),
            pltpu.VMEM((flat, columns), bf16),
            pltpu.VMEM((flat, columns), bf16),
            pltpu.VMEM((layers, rows), f32),
            pltpu.VMEM((layers, rows), f32),
            pltpu.VMEM((layers, columns), f32),
            pltpu.VMEM((layers, columns), f32),
            pltpu.VMEM((layers, columns), f32),
            pltpu.VMEM((nz, count, 8, LANES), f32),
            pltpu.VMEM((ny, layers, 8, columns), f32),
            pltpu.VMEM((ny, nz, 2, LANES), f32),
            pltpu.VMEM((nx, 2, LANES), f32),
            pltpu.VMEM((ny, nz, 2, LANES), f32),
            pltpu.VMEM((count, 8, LANES), f32),
            pltpu.VMEM((count, 8, LANES), f32),
            pltpu.VMEM((count, 8, LANES), f32),
            pltpu.VMEM((early, columns), f32),
            pltpu.VMEM((early, columns), bf16),
            pltpu.VMEM((layers, columns), f32),
            pltpu.VMEM((early, columns), bf16),
            sem(count),
            sem(count),
            sem(count),
            sem(2),
            sem(4),
            sem(5),
            sem(5),
            pltpu.SemaphoreType.DMA,
        ]
        + [sem(n) for n in pairs for _ in range(2)],
        compiler_params=pltpu.CompilerParams(
            collective_id=0, has_side_effects=True, vmem_limit_bytes=60 * 1024 * 1024
        ),
        cost_estimate=pl.CostEstimate(
            flops=20 * flat * columns, bytes_accessed=8 * flat * columns, transcendentals=0
        ),
    )(params.reshape(flat, columns), grads.reshape(flat, columns), row_state, col_state)


def place_kernel(
    late_chunks, chunk, from_hbm, late_hbm, row_in, col_in,
    out_hbm, row_out, col_out, stage, in_sem, out_sem,
):
    n, flat, columns = from_hbm.shape
    count, me = flat // chunk, lax.axis_index("gz")
    main = count - late_chunks
    row_out[...] = row_in[...]
    col_out[...] = col_in[...]

    def part(k):
        return pl.ds(pl.multiple_of(k * chunk, chunk), chunk)

    def copies(d, k, source):
        slot = d * count + k
        return (
            pltpu.make_async_copy(source, stage.at[d, part(k)], in_sem.at[slot]),
            pltpu.make_async_copy(
                stage.at[d, part(k)],
                out_hbm.at[part(k), pl.ds(d * columns, columns)],
                out_sem.at[slot],
            ),
        )

    def whole(act):
        for d in range(n):
            usual = lambda k, d=d: act(*copies(d, k, from_hbm.at[d, part(k)]))
            aside = lambda k, d=d: act(*copies(d, k, late_hbm.at[part(k - main)]))
            loop(0, main, usual)
            away = n - 1 - me if d == n - 1 else me if d == 0 else None
            if away is None:
                loop(main, count, usual)
            else:
                pl.when(away < n - 2)(lambda usual=usual: loop(main, count, usual))
                pl.when(away == n - 2)(lambda aside=aside: loop(main, count, aside))

    def relay(take, put):
        take.wait()
        put.start()

    whole(lambda take, put: take.start())
    whole(relay)
    whole(lambda take, put: put.wait())


def place(gathered, late, row_new, col_new, late_chunks, chunk):
    n, flat, columns = gathered.shape
    hbm, vmem = pl.BlockSpec(memory_space=pltpu.HBM), pl.BlockSpec(memory_space=pltpu.VMEM)
    slots = n * (flat // chunk)
    return pl.pallas_call(
        functools.partial(place_kernel, late_chunks, chunk),
        in_specs=[hbm, hbm, vmem, vmem],
        out_specs=(hbm, vmem, vmem),
        out_shape=(
            jax.ShapeDtypeStruct((flat, n * columns), bf16),
            jax.ShapeDtypeStruct(row_new.shape, f32),
            jax.ShapeDtypeStruct(col_new.shape, f32),
        ),
        scratch_shapes=[
            pltpu.VMEM((n, flat, columns), bf16),
            pltpu.SemaphoreType.DMA((slots,)),
            pltpu.SemaphoreType.DMA((slots,)),
        ],
        compiler_params=pltpu.CompilerParams(vmem_limit_bytes=56 * 1024 * 1024),
        cost_estimate=pl.CostEstimate(
            flops=n * flat * columns, bytes_accessed=4 * n * flat * columns, transcendentals=0
        ),
    )(gathered, late, row_new, col_new)


def place_late_kernel(n, held_hbm, moved, out_hbm, sem):
    rows, columns = moved.shape
    pieces = sem.shape[0]
    size, first = rows // pieces, out_hbm.shape[0] - rows
    for at, d in ((0, n - 1), (n - 1, 0)):

        @pl.when(lax.axis_index("gz") == at)
        def _(d=d):
            copies = [
                pltpu.make_async_copy(
                    moved.at[pl.ds(i * size, size)],
                    out_hbm.at[pl.ds(first + i * size, size), pl.ds(d * columns, columns)],
                    sem.at[i],
                )
                for i in range(pieces)
            ]
            for copy in copies:
                copy.start()
            for copy in copies:
                copy.wait()


def place_late(held, moved, n):
    anywhere = pl.BlockSpec(memory_space=pl.ANY)
    rows, columns = moved.shape
    return pl.pallas_call(
        functools.partial(place_late_kernel, n),
        in_specs=[anywhere, pl.BlockSpec(memory_space=pltpu.VMEM)],
        out_specs=anywhere,
        out_shape=jax.ShapeDtypeStruct(held.shape, bf16),
        scratch_shapes=[pltpu.SemaphoreType.DMA((rows // LANES,))],
        input_output_aliases={0: 0},
        compiler_params=pltpu.CompilerParams(vmem_limit_bytes=8 * 1024 * 1024),
        cost_estimate=pl.CostEstimate(
            flops=rows * columns, bytes_accessed=4 * rows * columns, transcendentals=0
        ),
    )(held, moved)


def body(params, grads, row_state, col_state):
    layers, rows, columns = params.shape
    n = lax.axis_size("gz")
    per, count, late_chunks, _ = cuts(layers, rows)
    row_new, col_new, row_root, col_step, gathered, late = step(
        params, grads, row_state, col_state
    )
    moved = lax.ppermute(late, "gz", [(n - 2, n - 1), (1, 0)])
    applied = grads.astype(f32) * row_root[:, :, None] * col_step[:, None, :]
    new_params = params - step_share * applied
    held, row_new, col_new = place(gathered, late, row_new, col_new, late_chunks, per * LANES)
    held = place_late(held, moved, n)
    compute = held.reshape(layers, rows, n * columns)
    return (new_params, row_new, col_new, applied, compute)


def solution(mesh):
    in_specs = (P("gx", "gy", "gz"), P("gx", "gy", "gz"), P("gx", "gy"), P("gx", "gz"))
    out_specs = (
        P("gx", "gy", "gz"),
        P("gx", "gy"),
        P("gx", "gz"),
        P("gx", "gy", "gz"),
        P("gx", "gy", None),
    )
    return jax.shard_map(body, mesh=mesh, in_specs=in_specs, out_specs=out_specs, check_vma=False)
```
